16 devices in a mesh: fsdp: 16 (over z, y, x, core).
Axes of the slice: x: 2, y: 2, z: 2, core: 2. Of those that a mesh axis runs over, the one named last changes fastest.
Arguments:
- hidden: bfloat16 [48, 512, 2048], P('fsdp')
- positions: int32 [48, 512], P('fsdp')
- grad_y: bfloat16 [48, 512, 2048], P('fsdp')
- attn_gain: bfloat16 [2048], P('fsdp')
- w_qkv: bfloat16 [2048, 3072], P('fsdp')
- b_qkv: bfloat16 [3072], P('fsdp')
- w_out: bfloat16 [2048, 2048], P('fsdp')
- mlp_gain: bfloat16 [2048], P('fsdp')
- w_up: bfloat16 [2048, 12288], P('fsdp')
- w_down: bfloat16 [6144, 2048], P('fsdp')
Outputs:
- output 1: bfloat16 [48, 512, 2048], P('fsdp')
- output 2: bfloat16 [48, 512, 2048], P('fsdp')
- output 3: float32 [2048], P('fsdp')
- output 4: float32 [2048, 3072], P('fsdp')
- output 5: float32 [3072], P('fsdp')
- output 6: float32 [2048, 2048], P('fsdp')
- output 7: float32 [2048], P('fsdp')
- output 8: float32 [2048, 12288], P('fsdp')
- output 9: float32 [6144, 2048], P('fsdp')
All inputs are finite; a program needn't handle non-finite values.
Results may differ from the reference program's by a relative error of at most 0.0161494.
Values are sent between devices in bfloat16 or wider.
A program may use at most 1 GiB of HBM per device.

```python
import jax
import jax.numpy as jnp
from jax import lax

H = 2048
HEADS = 16
KV_HEADS = 4
HEAD = 128
FF = 6144
BATCH = 48
SEQ = 512

QKV = (HEADS + 2 * KV_HEADS) * HEAD
Q_WIDTH = HEADS * HEAD
KV_WIDTH = KV_HEADS * HEAD
GROUP = HEADS // KV_HEADS
ROT_DIM = HEAD // 2
TOKENS = BATCH * SEQ
ROPE_BASE = 10000.0
EPS = 1e-5
SCALE = HEAD ** -0.5
CONTRACT_ROWS = (((0,), (0,)), ((), ()))
CONTRACT_COLS = (((1,), (1,)), ((), ()))


def setup_inputs(seed: int = 0) -> dict:
    rng_keys = jax.random.split(jax.random.key(seed), 11)
    hidden = jax.random.normal(rng_keys[0], (BATCH, SEQ, H), jnp.float32)
    pos_gaps = jax.random.randint(rng_keys[1], (BATCH, SEQ), 1, 4)
    starts = jax.random.randint(rng_keys[2], (BATCH, 1), 0, 64)
    positions = (starts + jnp.cumsum(pos_gaps, axis=1)).astype(jnp.int32)
    grad_y = jax.random.normal(rng_keys[3], (BATCH, SEQ, H), jnp.float32)
    attn_gain = 1.0 + 0.3 * jax.random.normal(rng_keys[4], (H,), jnp.float32)
    w_qkv = (1.5 * H ** -0.5) * jax.random.normal(rng_keys[5], (H, QKV), jnp.float32)
    b_qkv = 0.5 * jax.random.normal(rng_keys[6], (QKV,), jnp.float32)
    w_out = Q_WIDTH ** -0.5 * jax.random.normal(rng_keys[7], (Q_WIDTH, H), jnp.float32)
    mlp_gain = 1.0 + 0.3 * jax.random.normal(rng_keys[8], (H,), jnp.float32)
    w_up = H ** -0.5 * jax.random.normal(rng_keys[9], (H, 2 * FF), jnp.float32)
    w_down = FF ** -0.5 * jax.random.normal(rng_keys[10], (FF, H), jnp.float32)
    return {
        'hidden': hidden.astype(jnp.bfloat16),
        'positions': positions,
        'grad_y': grad_y.astype(jnp.bfloat16),
        'attn_gain': attn_gain.astype(jnp.bfloat16),
        'w_qkv': w_qkv.astype(jnp.bfloat16),
        'b_qkv': b_qkv.astype(jnp.bfloat16),
        'w_out': w_out.astype(jnp.bfloat16),
        'mlp_gain': mlp_gain.astype(jnp.bfloat16),
        'w_up': w_up.astype(jnp.bfloat16),
        'w_down': w_down.astype(jnp.bfloat16),
    }


def norm_scale(rows_in):
    return lax.rsqrt(jnp.mean(rows_in * rows_in, axis=-1, keepdims=True) + EPS)


def rope_turn(head_vals, cos_t, sin_t):
    lead_shape = head_vals.shape[:-1]
    rot_pairs = head_vals[..., :ROT_DIM].reshape(lead_shape + (ROT_DIM // 2, 2))
    even_part = rot_pairs[..., 0]
    odd_part = rot_pairs[..., 1]
    turned = jnp.stack([even_part * cos_t - odd_part * sin_t, odd_part * cos_t + even_part * sin_t], axis=-1)
    return jnp.concatenate([turned.reshape(lead_shape + (ROT_DIM,)), head_vals[..., ROT_DIM:]], axis=-1)


def causal_mask():
    token_index = jnp.arange(SEQ)
    return token_index[:, None] >= token_index[None, :]


def attend_forward(operands):
    q_rot, k_rot, values = operands
    scores = jnp.einsum('qkgd,skd->kgqs', q_rot.astype(jnp.float32), k_rot.astype(jnp.float32)) * SCALE
    attn_probs = jax.nn.softmax(jnp.where(causal_mask(), scores, -1e30), axis=-1)
    context = jnp.einsum('kgqs,skd->qkgd', attn_probs.astype(jnp.bfloat16).astype(jnp.float32), values.astype(jnp.float32))
    return context.astype(jnp.bfloat16)


def attend_backward(operands):
    q_rot, k_rot, values, d_context = operands
    q_wide = q_rot.astype(jnp.float32)
    k_wide = k_rot.astype(jnp.float32)
    v_wide = values.astype(jnp.float32)
    dc_wide = d_context.astype(jnp.float32)
    scores = jnp.einsum('qkgd,skd->kgqs', q_wide, k_wide) * SCALE
    attn_probs = jax.nn.softmax(jnp.where(causal_mask(), scores, -1e30), axis=-1)
    d_probs = jnp.einsum('qkgd,skd->kgqs', dc_wide, v_wide)
    d_values = jnp.einsum('kgqs,qkgd->skd', attn_probs.astype(jnp.bfloat16).astype(jnp.float32), dc_wide)
    d_scores = attn_probs * (d_probs - jnp.sum(attn_probs * d_probs, axis=-1, keepdims=True)) * SCALE
    ds_wide = d_scores.astype(jnp.bfloat16).astype(jnp.float32)
    d_query = jnp.einsum('kgqs,skd->qkgd', ds_wide, k_wide)
    d_key = jnp.einsum('kgqs,qkgd->skd', ds_wide, q_wide)
    return d_query, d_key, d_values


def reference(hidden, positions, grad_y, attn_gain, w_qkv, b_qkv, w_out, mlp_gain, w_up, w_down):
    inv_freq = 1.0 / (ROPE_BASE ** (jnp.arange(0, ROT_DIM, 2, dtype=jnp.float32) / ROT_DIM))
    angles = positions.astype(jnp.float32)[:, :, None, None] * inv_freq
    cos_t = jnp.cos(angles)
    sin_t = jnp.sin(angles)
    hid_wide = hidden.reshape(TOKENS, H).astype(jnp.float32)
    inv_one = norm_scale(hid_wide)
    gain_one = attn_gain.astype(jnp.float32)
    normed = (hid_wide * inv_one * gain_one).astype(jnp.bfloat16)
    qkv_proj = jnp.dot(normed, w_qkv, preferred_element_type=jnp.float32) + b_qkv.astype(jnp.float32)
    qkv_proj = qkv_proj.reshape(BATCH, SEQ, QKV)
    q_rot = rope_turn(qkv_proj[..., :Q_WIDTH].reshape(BATCH, SEQ, HEADS, HEAD), cos_t, sin_t)
    q_rot = q_rot.astype(jnp.bfloat16).reshape(BATCH, SEQ, KV_HEADS, GROUP, HEAD)
    k_rot = rope_turn(qkv_proj[..., Q_WIDTH:Q_WIDTH + KV_WIDTH].reshape(BATCH, SEQ, KV_HEADS, HEAD), cos_t, sin_t).astype(jnp.bfloat16)
    values = qkv_proj[..., Q_WIDTH + KV_WIDTH:].reshape(BATCH, SEQ, KV_HEADS, HEAD).astype(jnp.bfloat16)
    context = lax.map(attend_forward, (q_rot, k_rot, values)).reshape(TOKENS, Q_WIDTH)
    mid_state = (hid_wide + jnp.dot(context, w_out, preferred_element_type=jnp.float32)).astype(jnp.bfloat16)
    mid_wide = mid_state.astype(jnp.float32)
    inv_two = norm_scale(mid_wide)
    gain_two = mlp_gain.astype(jnp.float32)
    mlp_in = (mid_wide * inv_two * gain_two).astype(jnp.bfloat16)
    up_all = jnp.dot(mlp_in, w_up, preferred_element_type=jnp.float32).astype(jnp.bfloat16)
    gate_val = up_all[:, :FF].astype(jnp.float32)
    lin_val = up_all[:, FF:].astype(jnp.float32)
    sigmoid_gate = jax.nn.sigmoid(gate_val)
    act_val = (gate_val * sigmoid_gate * lin_val).astype(jnp.bfloat16)
    output = (mid_wide + jnp.dot(act_val, w_down, preferred_element_type=jnp.float32)).astype(jnp.bfloat16)

    dy_flat = grad_y.reshape(TOKENS, H)
    grad_w_down = lax.dot_general(act_val, dy_flat, CONTRACT_ROWS, preferred_element_type=jnp.float32)
    d_act = lax.dot_general(dy_flat, w_down, CONTRACT_COLS, preferred_element_type=jnp.float32)
    d_gate = d_act * lin_val * sigmoid_gate * (1.0 + gate_val * (1.0 - sigmoid_gate))
    d_lin = d_act * gate_val * sigmoid_gate
    d_up = jnp.concatenate([d_gate, d_lin], axis=1).astype(jnp.bfloat16)
    grad_w_up = lax.dot_general(mlp_in, d_up, CONTRACT_ROWS, preferred_element_type=jnp.float32)
    d_mlp_in = lax.dot_general(d_up, w_up, CONTRACT_COLS, preferred_element_type=jnp.float32)
    grad_mlp_gain = jnp.sum(d_mlp_in * mid_wide * inv_two, axis=0)
    scaled_two = d_mlp_in * gain_two
    d_mid = dy_flat.astype(jnp.float32) + inv_two * (scaled_two - mid_wide * inv_two * inv_two * jnp.mean(scaled_two * mid_wide, axis=-1, keepdims=True))
    d_mid_low = d_mid.astype(jnp.bfloat16)
    grad_w_out = lax.dot_general(context, d_mid_low, CONTRACT_ROWS, preferred_element_type=jnp.float32)
    d_context = lax.dot_general(d_mid_low, w_out, CONTRACT_COLS, preferred_element_type=jnp.float32)
    d_context = d_context.astype(jnp.bfloat16).reshape(BATCH, SEQ, KV_HEADS, GROUP, HEAD)
    d_query, d_key, d_values = lax.map(attend_backward, (q_rot, k_rot, values, d_context))
    d_query = rope_turn(d_query.reshape(BATCH, SEQ, HEADS, HEAD), cos_t, -sin_t)
    d_key = rope_turn(d_key, cos_t, -sin_t)
    d_proj = jnp.concatenate([d_query.reshape(TOKENS, Q_WIDTH), d_key.reshape(TOKENS, KV_WIDTH), d_values.reshape(TOKENS, KV_WIDTH)], axis=1)
    grad_b_qkv = jnp.sum(d_proj, axis=0)
    d_proj_low = d_proj.astype(jnp.bfloat16)
    grad_w_qkv = lax.dot_general(normed, d_proj_low, CONTRACT_ROWS, preferred_element_type=jnp.float32)
    d_normed = lax.dot_general(d_proj_low, w_qkv, CONTRACT_COLS, preferred_element_type=jnp.float32)
    grad_attn_gain = jnp.sum(d_normed * hid_wide * inv_one, axis=0)
    scaled_one = d_normed * gain_one
    grad_hidden = (d_mid + inv_one * (scaled_one - hid_wide * inv_one * inv_one * jnp.mean(scaled_one * hid_wide, axis=-1, keepdims=True))).astype(jnp.bfloat16)
    return (output.reshape(BATCH, SEQ, H), grad_hidden.reshape(BATCH, SEQ, H), grad_attn_gain, grad_w_qkv, grad_b_qkv, grad_w_out, grad_mlp_gain, grad_w_up, grad_w_down)
```

```python
import jax
import jax.numpy as jnp
from jax import lax
from jax.sharding import PartitionSpec as P

HEAD_DIM = 128
ROPE_BASE = 10000.0
EPS = 1e-5


def norm_scale(rows_in):
    return lax.rsqrt(jnp.mean(rows_in * rows_in, axis=-1, keepdims=True) + EPS)


def rope_tables(positions):
    rot_dim = HEAD_DIM // 2
    inv_freq = 1.0 / (ROPE_BASE ** (jnp.arange(0, rot_dim, 2, dtype=jnp.float32) / rot_dim))
    angles = positions.astype(jnp.float32)[:, :, None, None] * inv_freq
    return jnp.cos(angles), jnp.sin(angles)


def rope_turn(head_vals, cos_t, sin_t):
    rot_dim = HEAD_DIM // 2
    lead_shape = head_vals.shape[:-1]
    rot_pairs = head_vals[..., :rot_dim].reshape(lead_shape + (rot_dim // 2, 2))
    even_part = rot_pairs[..., 0]
    odd_part = rot_pairs[..., 1]
    turned = jnp.stack([even_part * cos_t - odd_part * sin_t, odd_part * cos_t + even_part * sin_t], axis=-1)
    return jnp.concatenate([turned.reshape(lead_shape + (rot_dim,)), head_vals[..., rot_dim:]], axis=-1)


def attend_forward(q_rot, k_rot, values):
    seq_len = q_rot.shape[1]
    token_index = jnp.arange(seq_len)
    causal = token_index[:, None] >= token_index[None, :]
    scores = jnp.einsum('bqkgd,bskd->bkgqs', q_rot, k_rot, preferred_element_type=jnp.float32) * HEAD_DIM ** -0.5
    attn_probs = jax.nn.softmax(jnp.where(causal, scores, -1e30), axis=-1)
    probs_low = attn_probs.astype(jnp.bfloat16)
    context = jnp.einsum('bkgqs,bskd->bqkgd', probs_low, values, preferred_element_type=jnp.float32)
    return context.astype(jnp.bfloat16), attn_probs, probs_low


def attend_backward(q_rot, k_rot, values, attn_probs, probs_low, d_context):
    d_probs = jnp.einsum('bqkgd,bskd->bkgqs', d_context, values, preferred_element_type=jnp.float32)
    d_values = jnp.einsum('bkgqs,bqkgd->bskd', probs_low, d_context, preferred_element_type=jnp.float32)
    d_scores = attn_probs * (d_probs - jnp.sum(attn_probs * d_probs, axis=-1, keepdims=True)) * HEAD_DIM ** -0.5
    d_scores = d_scores.astype(jnp.bfloat16)
    d_query = jnp.einsum('bkgqs,bskd->bqkgd', d_scores, k_rot, preferred_element_type=jnp.float32)
    d_key = jnp.einsum('bkgqs,bqkgd->bskd', d_scores, q_rot, preferred_element_type=jnp.float32)
    return d_query, d_key, d_values


def own_blocks(rows_in, width, bit):
    return jnp.concatenate([lax.dynamic_slice_in_dim(rows_in, (2 * i + bit) * width, width, axis=1) for i in range(8)], axis=1)


def outer_sum(own_left, own_right, far_left, far_right):
    first = lax.dot_general(own_left, own_right, CONTRACT_ROWS, preferred_element_type=jnp.float32)
    return first + lax.dot_general(far_left, far_right, CONTRACT_ROWS, preferred_element_type=jnp.float32)


CONTRACT_ROWS = (((0,), (0,)), ((), ()))
CONTRACT_COLS = (((1,), (1,)), ((), ()))


def layer_pass(axis, hidden, positions, grad_y, attn_gain_s, w_qkv_s, b_qkv_s, w_out_s, mlp_gain_s, w_up_s, w_down_s):
    batch_size, seq_len, width = hidden.shape
    tokens = batch_size * seq_len
    count = lax.axis_size(axis)
    bit = lax.axis_index(axis) % 2
    swap = [(i, i ^ 1) for i in range(count)]
    groups = [list(range(0, count, 2)), list(range(1, count, 2))]

    def far(value):
        return lax.ppermute(value, axis, swap)

    def scatter(chip_sum):
        return lax.psum_scatter(chip_sum, axis, scatter_dimension=0, axis_index_groups=groups, tiled=True)

    def gather(shard):
        return lax.all_gather(shard, axis, axis=0, tiled=True)

    gain_rows = attn_gain_s.shape[0]
    bias_rows = b_qkv_s.shape[0]
    packed = jnp.concatenate([attn_gain_s, mlp_gain_s, b_qkv_s, jnp.zeros((4 * 128 - 2 * gain_rows - bias_rows,), jnp.bfloat16)])
    packed = lax.all_gather(packed.reshape(1, 4, 128), axis, axis=0, tiled=True).reshape(count, 512)
    attn_gain = packed[:, :gain_rows].reshape(width)
    mlp_gain = packed[:, gain_rows:2 * gain_rows].reshape(width)
    b_qkv = packed[:, 2 * gain_rows:2 * gain_rows + bias_rows].reshape(bias_rows * count)
    w_qkv = gather(w_qkv_s)
    w_out = gather(w_out_s)
    w_up = gather(w_up_s)
    w_down = gather(w_down_s)

    q_width = w_out.shape[0]
    kv_width = (w_qkv.shape[1] - q_width) // 2
    kv_heads = kv_width // HEAD_DIM
    group_size = q_width // kv_width
    ff_width = w_down.shape[0]
    cos_t, sin_t = rope_tables(positions)
    dy = grad_y.reshape(tokens, width)
    hid_wide = hidden.reshape(tokens, width).astype(jnp.float32)
    inv_one = norm_scale(hid_wide)
    gain_one = attn_gain.astype(jnp.float32)
    normed = (hid_wide * inv_one * gain_one).astype(jnp.bfloat16)
    far_dy = far(dy)
    qkv_proj = jnp.dot(normed, w_qkv, preferred_element_type=jnp.float32) + b_qkv.astype(jnp.float32)
    qkv_proj = qkv_proj.reshape(batch_size, seq_len, -1)
    q_rot = rope_turn(qkv_proj[..., :q_width].reshape(batch_size, seq_len, q_width // HEAD_DIM, HEAD_DIM), cos_t, sin_t)
    q_rot = q_rot.astype(jnp.bfloat16).reshape(batch_size, seq_len, kv_heads, group_size, HEAD_DIM)
    k_rot = rope_turn(qkv_proj[..., q_width:q_width + kv_width].reshape(batch_size, seq_len, kv_heads, HEAD_DIM), cos_t, sin_t).astype(jnp.bfloat16)
    values = qkv_proj[..., q_width + kv_width:].reshape(batch_size, seq_len, kv_heads, HEAD_DIM).astype(jnp.bfloat16)
    context, attn_probs, probs_low = attend_forward(q_rot, k_rot, values)
    context = context.reshape(tokens, q_width)
    mid_state = (hid_wide + jnp.dot(context, w_out, preferred_element_type=jnp.float32)).astype(jnp.bfloat16)
    mid_wide = mid_state.astype(jnp.float32)
    inv_two = norm_scale(mid_wide)
    gain_two = mlp_gain.astype(jnp.float32)
    mlp_in = (mid_wide * inv_two * gain_two).astype(jnp.bfloat16)
    up_all = jnp.dot(mlp_in, w_up, preferred_element_type=jnp.float32).astype(jnp.bfloat16)
    gate_val = up_all[..., :ff_width].astype(jnp.float32)
    lin_val = up_all[..., ff_width:].astype(jnp.float32)
    sigmoid_gate = jax.nn.sigmoid(gate_val)
    act_val = (gate_val * sigmoid_gate * lin_val).astype(jnp.bfloat16)

    ff_rows = ff_width // count
    own_act = own_blocks(act_val, ff_rows, bit)
    far_act = far(own_blocks(act_val, ff_rows, 1 - bit))
    chip_w_down = outer_sum(own_act, dy, far_act, far_dy)
    chip_w_down, dy_next = lax.optimization_barrier((chip_w_down, dy))
    grad_w_down = scatter(chip_w_down)

    d_act = lax.dot_general(dy_next, w_down, CONTRACT_COLS, preferred_element_type=jnp.float32)
    d_gate = (d_act * lin_val * sigmoid_gate * (1.0 + gate_val * (1.0 - sigmoid_gate))).astype(jnp.bfloat16)
    d_lin = (d_act * gate_val * sigmoid_gate).astype(jnp.bfloat16)
    far_gate = far(d_gate)
    far_lin = far(d_lin)
    h_rows = width // count
    own_mlp = own_blocks(mlp_in, h_rows, bit)
    far_mlp = far(own_blocks(mlp_in, h_rows, 1 - bit))
    d_up = jnp.concatenate([d_gate, d_lin], axis=-1)
    far_up = jnp.concatenate([far_gate, far_lin], axis=-1)
    chip_w_up = outer_sum(own_mlp, d_up, far_mlp, far_up)
    chip_w_up, d_up_next = lax.optimization_barrier((chip_w_up, d_up))
    grad_w_up = scatter(chip_w_up)

    d_mlp_in = lax.dot_general(d_up_next, w_up, CONTRACT_COLS, preferred_element_type=jnp.float32)
    grad_mlp_gain = jnp.sum(d_mlp_in * mid_wide * inv_two, axis=0)
    scaled_two = d_mlp_in * gain_two
    d_mid = dy.astype(jnp.float32) + inv_two * (scaled_two - mid_wide * inv_two * inv_two * jnp.mean(scaled_two * mid_wide, axis=-1, keepdims=True))
    d_mid_low = d_mid.astype(jnp.bfloat16)
    far_mid = far(d_mid_low)
    own_ctx = own_blocks(context, q_width // count, bit)
    far_ctx = far(own_blocks(context, q_width // count, 1 - bit))
    d_context = lax.dot_general(d_mid_low, w_out, CONTRACT_COLS, preferred_element_type=jnp.float32)
    d_context = d_context.astype(jnp.bfloat16)
    chip_w_out = outer_sum(own_ctx, d_mid_low, far_ctx, far_mid)
    chip_w_out, d_context = lax.optimization_barrier((chip_w_out, d_context))
    grad_w_out = scatter(chip_w_out)
    d_context = d_context.reshape(batch_size, seq_len, kv_heads, group_size, HEAD_DIM)
    d_query, d_key, d_values = attend_backward(q_rot, k_rot, values, attn_probs, probs_low, d_context)
    d_query = rope_turn(d_query.reshape(batch_size, seq_len, q_width // HEAD_DIM, HEAD_DIM), cos_t, -sin_t)
    d_key = rope_turn(d_key, cos_t, -sin_t)
    d_proj = jnp.concatenate([d_query.reshape(tokens, q_width), d_key.reshape(tokens, kv_width), d_values.reshape(tokens, kv_width)], axis=-1)
    grad_b_qkv = jnp.sum(d_proj, axis=0)
    d_proj_low = d_proj.astype(jnp.bfloat16)
    far_proj = far(d_proj_low)
    own_normed = own_blocks(normed, h_rows, bit)
    far_normed = far(own_blocks(normed, h_rows, 1 - bit))
    chip_w_qkv = outer_sum(own_normed, d_proj_low, far_normed, far_proj)
    chip_w_qkv, d_proj_next, act_next = lax.optimization_barrier((chip_w_qkv, d_proj_low, act_val))
    grad_w_qkv = scatter(chip_w_qkv)
    d_normed = lax.dot_general(d_proj_next, w_qkv, CONTRACT_COLS, preferred_element_type=jnp.float32)
    grad_attn_gain = jnp.sum(d_normed * hid_wide * inv_one, axis=0)
    scaled_one = d_normed * gain_one
    grad_hidden = (d_mid + inv_one * (scaled_one - hid_wide * inv_one * inv_one * jnp.mean(scaled_one * hid_wide, axis=-1, keepdims=True))).astype(jnp.bfloat16)
    output = (mid_wide + jnp.dot(act_next, w_down, preferred_element_type=jnp.float32)).astype(jnp.bfloat16)

    small = [lax.psum_scatter(value, axis, scatter_dimension=0, tiled=True) for value in (grad_attn_gain, grad_b_qkv, grad_mlp_gain)]
    whole = (batch_size, seq_len, width)
    return output.reshape(whole), grad_hidden.reshape(whole), small[0], grad_w_qkv, small[1], grad_w_out, small[2], grad_w_up, grad_w_down


def solution(mesh):
    group_axis = mesh.axis_names[0]

    def local_step(*args):
        return layer_pass(group_axis, *args)

    row_spec = P(group_axis)
    return jax.shard_map(local_step, mesh=mesh, in_specs=(row_spec,) * 10, out_specs=(row_spec,) * 9, check_vma=False)
```

```python
import functools

import jax
import jax.numpy as jnp
from jax import lax
from jax.experimental import pallas as pl
from jax.experimental.pallas import tpu as pltpu
from jax.sharding import PartitionSpec as P


HEAD_DIM = 128
ROT_DIM = 64
ROPE_BASE = 10000.0
EPS = 1e-5
BLOCK = 128
CONTRACT_ROWS = (((0,), (0,)), ((), ()))
CONTRACT_COLS = (((1,), (1,)), ((), ()))


def norm_scale(rows_in):
    return lax.rsqrt(jnp.mean(rows_in * rows_in, axis=-1, keepdims=True) + EPS)


def rope_tables(positions):
    inv_freq = 1.0 / (ROPE_BASE ** (jnp.arange(0, ROT_DIM, 2, dtype=jnp.float32) / ROT_DIM))
    lane_freq = jnp.concatenate([jnp.repeat(inv_freq, 2), jnp.zeros((HEAD_DIM - ROT_DIM,), jnp.float32)])
    angles = positions.reshape(-1, 1).astype(jnp.float32) * lane_freq
    signs = jnp.where(jnp.arange(HEAD_DIM) % 2 == 0, -1.0, 1.0)
    return jnp.cos(angles), jnp.sin(angles) * signs


def turn(head_vals, cos_t, sin_t):
    lane = lax.broadcasted_iota(jnp.int32, head_vals.shape, 1)
    partner = jnp.where(lane % 2 == 0, pltpu.roll(head_vals, HEAD_DIM - 1, 1), pltpu.roll(head_vals, 1, 1))
    return jnp.where(lane < ROT_DIM, head_vals * cos_t + partner * sin_t, head_vals)


def probs_t(keys, queries, first_row):
    scores = lax.dot_general(keys, queries, CONTRACT_COLS, preferred_element_type=jnp.float32) * HEAD_DIM ** -0.5
    key_at = lax.broadcasted_iota(jnp.int32, scores.shape, 0)
    query_at = lax.broadcasted_iota(jnp.int32, scores.shape, 1) % BLOCK + first_row
    scores = jnp.where(query_at >= key_at, scores, -1e30)
    weights = jnp.exp(scores - jnp.max(scores, axis=0, keepdims=True))
    return weights * (1.0 / jnp.sum(weights, axis=0, keepdims=True))


def attend_kernel(heads, kv_heads, z_ref, cos_ref, sin_ref, rot_ref, ctx_ref):
    seq = z_ref.shape[0]
    group = heads // kv_heads

    @pl.loop(0, heads + kv_heads)
    def _(j):
        at = pl.ds(pl.multiple_of(j * HEAD_DIM, HEAD_DIM), HEAD_DIM)
        rot_ref[:, at] = turn(z_ref[:, at], cos_ref[...], sin_ref[...]).astype(jnp.bfloat16)

    v_at = (heads + kv_heads) * HEAD_DIM
    rot_ref[:, v_at:] = z_ref[:, v_at:].astype(jnp.bfloat16)

    @pl.loop(0, kv_heads)
    def _(j):
        def head_at(n):
            return pl.ds(pl.multiple_of(n * HEAD_DIM, HEAD_DIM), HEAD_DIM)

        for first in range(0, seq, BLOCK):
            last = first + BLOCK
            queries = jnp.concatenate([rot_ref[first:last, head_at(j * group + g)] for g in range(group)], axis=0)
            probs = probs_t(rot_ref[:last, head_at(heads + j)], queries, first).astype(jnp.bfloat16)
            ctx = lax.dot_general(probs, rot_ref[:last, head_at(heads + kv_heads + j)], CONTRACT_ROWS, preferred_element_type=jnp.float32)
            for g in range(group):
                ctx_ref[first:last, head_at(j * group + g)] = ctx[g * BLOCK:(g + 1) * BLOCK].astype(jnp.bfloat16)


def attend_grad_kernel(heads, kv_heads, rot_ref, dctx_ref, cos_ref, sin_ref, dz_ref, bias_ref, dk_ref, dv_ref):
    seq = rot_ref.shape[0]
    group = heads // kv_heads

    @pl.loop(0, kv_heads)
    def _(j):
        def head_at(n):
            return pl.ds(pl.multiple_of(n * HEAD_DIM, HEAD_DIM), HEAD_DIM)

        def put(rows, head, value, fresh):
            dz_ref[rows, head_at(head)] = value.astype(jnp.bfloat16)
            part = jnp.sum(value.reshape(-1, 8, HEAD_DIM), axis=0)
            if fresh:
                bias_ref[0, :, head_at(head)] = part
            else:
                bias_ref[0, :, head_at(head)] += part

        dk_ref[...] = jnp.zeros_like(dk_ref)
        dv_ref[...] = jnp.zeros_like(dv_ref)
        for first in range(0, seq, BLOCK):
            last = first + BLOCK
            rows = slice(first, last)
            queries = jnp.concatenate([rot_ref[rows, head_at(j * group + g)] for g in range(group)], axis=0)
            dctx = jnp.concatenate([dctx_ref[rows, head_at(j * group + g)] for g in range(group)], axis=0)
            keys = rot_ref[:last, head_at(heads + j)]
            probs = probs_t(keys, queries, first)
            dv_ref[:last] += jnp.dot(probs.astype(jnp.bfloat16), dctx, preferred_element_type=jnp.float32)
            d_probs = lax.dot_general(rot_ref[:last, head_at(heads + kv_heads + j)], dctx, CONTRACT_COLS, preferred_element_type=jnp.float32)
            inner = jnp.sum(probs * d_probs, axis=0, keepdims=True)
            d_scores = (probs * (d_probs - inner) * HEAD_DIM ** -0.5).astype(jnp.bfloat16)
            dk_ref[:last] += jnp.dot(d_scores, queries, preferred_element_type=jnp.float32)
            d_query = lax.dot_general(d_scores, keys, CONTRACT_ROWS, preferred_element_type=jnp.float32)
            for g in range(group):
                turned = turn(d_query[g * BLOCK:(g + 1) * BLOCK], cos_ref[rows], -sin_ref[rows])
                put(rows, j * group + g, turned, first == 0)
        put(slice(0, seq), heads + j, turn(dk_ref[...], cos_ref[...], -sin_ref[...]), True)
        put(slice(0, seq), heads + kv_heads + j, dv_ref[...], True)


def rows_spec(seq, width):
    return pl.BlockSpec((seq, width), lambda i: (i, 0))


def attend(qkv_proj, cos_t, sin_t, seq, heads, kv_heads):
    tokens, width = qkv_proj.shape
    q_width = heads * HEAD_DIM
    return pl.pallas_call(
        functools.partial(attend_kernel, heads, kv_heads),
        grid=(tokens // seq,),
        in_specs=[rows_spec(seq, width), rows_spec(seq, HEAD_DIM), rows_spec(seq, HEAD_DIM)],
        out_specs=[rows_spec(seq, width), rows_spec(seq, q_width)],
        out_shape=[jax.ShapeDtypeStruct((tokens, width), jnp.bfloat16), jax.ShapeDtypeStruct((tokens, q_width), jnp.bfloat16)],
        cost_estimate=pl.CostEstimate(flops=30_000_000_000, bytes_accessed=40_000_000, transcendentals=10_000_000),
    )(qkv_proj, cos_t, sin_t)


def attend_grad(rot, d_context, cos_t, sin_t, seq, heads, kv_heads):
    tokens, width = rot.shape
    count = tokens // seq
    return pl.pallas_call(
        functools.partial(attend_grad_kernel, heads, kv_heads),
        grid=(count,),
        in_specs=[rows_spec(seq, width), rows_spec(seq, heads * HEAD_DIM), rows_spec(seq, HEAD_DIM), rows_spec(seq, HEAD_DIM)],
        out_specs=[rows_spec(seq, width), pl.BlockSpec((1, 8, width), lambda i: (i, 0, 0))],
        out_shape=[jax.ShapeDtypeStruct((tokens, width), jnp.bfloat16), jax.ShapeDtypeStruct((count, 8, width), jnp.float32)],
        scratch_shapes=[pltpu.VMEM((seq, HEAD_DIM), jnp.float32), pltpu.VMEM((seq, HEAD_DIM), jnp.float32)],
        cost_estimate=pl.CostEstimate(flops=60_000_000_000, bytes_accessed=40_000_000, transcendentals=10_000_000),
    )(rot, d_context, cos_t, sin_t)


def own_blocks(rows_in, width, bit):
    return jnp.concatenate([lax.dynamic_slice_in_dim(rows_in, (2 * i + bit) * width, width, axis=1) for i in range(8)], axis=1)


def outer_sum(own_left, own_right, far_left, far_right):
    first = lax.dot_general(own_left, own_right, CONTRACT_ROWS, preferred_element_type=jnp.float32)
    return first + lax.dot_general(far_left, far_right, CONTRACT_ROWS, preferred_element_type=jnp.float32)


def layer_pass(axis, hidden, positions, grad_y, attn_gain_s, w_qkv_s, b_qkv_s, w_out_s, mlp_gain_s, w_up_s, w_down_s):
    batch_size, seq_len, width = hidden.shape
    tokens = batch_size * seq_len
    count = lax.axis_size(axis)
    bit = lax.axis_index(axis) % 2
    swap = [(i, i ^ 1) for i in range(count)]
    groups = [list(range(0, count, 2)), list(range(1, count, 2))]

    def far(value):
        return lax.ppermute(value, axis, swap)

    def scatter(chip_sum):
        return lax.psum_scatter(chip_sum, axis, scatter_dimension=0, axis_index_groups=groups, tiled=True)

    def gather(shard):
        return lax.all_gather(shard, axis, axis=0, tiled=True)

    gain_rows = attn_gain_s.shape[0]
    bias_rows = b_qkv_s.shape[0]
    packed = jnp.concatenate([attn_gain_s, mlp_gain_s, b_qkv_s, jnp.zeros((4 * 128 - 2 * gain_rows - bias_rows,), jnp.bfloat16)])
    packed = lax.all_gather(packed.reshape(1, 4, 128), axis, axis=0, tiled=True).reshape(count, 512)
    attn_gain = packed[:, :gain_rows].reshape(width)
    mlp_gain = packed[:, gain_rows:2 * gain_rows].reshape(width)
    b_qkv = packed[:, 2 * gain_rows:2 * gain_rows + bias_rows].reshape(bias_rows * count)
    ff_width = w_down_s.shape[0] * count
    w_qkv = gather(w_qkv_s)
    w_out = gather(w_out_s)
    w_gate = gather(w_up_s[:, :ff_width])
    w_lin = gather(w_up_s[:, ff_width:])
    w_down = gather(w_down_s)

    q_width = w_out.shape[0]
    kv_width = (w_qkv.shape[1] - q_width) // 2
    heads = q_width // HEAD_DIM
    kv_heads = kv_width // HEAD_DIM
    h_rows = width // count
    ff_rows = ff_width // count
    cos_t, sin_t = rope_tables(positions)
    dy = grad_y.reshape(tokens, width)
    hid_wide = hidden.reshape(tokens, width).astype(jnp.float32)
    inv_one = norm_scale(hid_wide)
    gain_one = attn_gain.astype(jnp.float32)
    normed = (hid_wide * inv_one * gain_one).astype(jnp.bfloat16)
    far_dy = far(dy)
    own_normed = own_blocks(normed, h_rows, bit)
    far_normed = far(own_blocks(normed, h_rows, 1 - bit))
    qkv_proj = jnp.dot(normed, w_qkv, preferred_element_type=jnp.float32) + b_qkv.astype(jnp.float32)
    rot, context = attend(qkv_proj, cos_t, sin_t, seq_len, heads, kv_heads)
    mid_state = (hid_wide + jnp.dot(context, w_out, preferred_element_type=jnp.float32)).astype(jnp.bfloat16)
    mid_wide = mid_state.astype(jnp.float32)
    inv_two = norm_scale(mid_wide)
    gain_two = mlp_gain.astype(jnp.float32)
    mlp_in = (mid_wide * inv_two * gain_two).astype(jnp.bfloat16)
    own_mlp = own_blocks(mlp_in, h_rows, bit)
    far_mlp = far(own_blocks(mlp_in, h_rows, 1 - bit))
    own_ctx = own_blocks(context, q_width // count, bit)
    far_ctx = far(own_blocks(context, q_width // count, 1 - bit))
    up_gate = jnp.dot(mlp_in, w_gate, preferred_element_type=jnp.float32).astype(jnp.bfloat16)
    up_lin = jnp.dot(mlp_in, w_lin, preferred_element_type=jnp.float32).astype(jnp.bfloat16)
    gate_val = up_gate.astype(jnp.float32)
    lin_val = up_lin.astype(jnp.float32)
    sigmoid_gate = jax.nn.sigmoid(gate_val)
    act_val = (gate_val * sigmoid_gate * lin_val).astype(jnp.bfloat16)

    own_act = own_blocks(act_val, ff_rows, bit)
    far_act = far(own_blocks(act_val, ff_rows, 1 - bit))
    chip_w_down = outer_sum(own_act, dy, far_act, far_dy)
    chip_w_down, dy_next = lax.optimization_barrier((chip_w_down, dy))
    grad_w_down = scatter(chip_w_down)

    d_act = lax.dot_general(dy_next, w_down, CONTRACT_COLS, preferred_element_type=jnp.float32)
    d_gate = (d_act * lin_val * sigmoid_gate * (1.0 + gate_val * (1.0 - sigmoid_gate))).astype(jnp.bfloat16)
    d_lin = (d_act * gate_val * sigmoid_gate).astype(jnp.bfloat16)
    chip_w_gate = outer_sum(own_mlp, d_gate, far_mlp, far(d_gate))
    chip_w_lin = outer_sum(own_mlp, d_lin, far_mlp, far(d_lin))
    chip_w_gate, chip_w_lin, d_gate_next, d_lin_next, grad_w_down = lax.optimization_barrier((chip_w_gate, chip_w_lin, d_gate, d_lin, grad_w_down))
    grad_w_gate = scatter(chip_w_gate)
    grad_w_lin = scatter(chip_w_lin)

    d_mlp_in = lax.dot_general(d_gate_next, w_gate, CONTRACT_COLS, preferred_element_type=jnp.float32)
    d_mlp_in = d_mlp_in + lax.dot_general(d_lin_next, w_lin, CONTRACT_COLS, preferred_element_type=jnp.float32)
    grad_mlp_gain = jnp.sum(d_mlp_in * mid_wide * inv_two, axis=0)
    scaled_two = d_mlp_in * gain_two
    d_mid = dy.astype(jnp.float32) + inv_two * (scaled_two - mid_wide * inv_two * inv_two * jnp.mean(scaled_two * mid_wide, axis=-1, keepdims=True))
    d_mid_low = d_mid.astype(jnp.bfloat16)
    d_context = lax.dot_general(d_mid_low, w_out, CONTRACT_COLS, preferred_element_type=jnp.float32).astype(jnp.bfloat16)
    chip_w_out = outer_sum(own_ctx, d_mid_low, far_ctx, far(d_mid_low))
    d_proj_low, bias_parts = attend_grad(rot, d_context, cos_t, sin_t, seq_len, heads, kv_heads)
    grad_b_qkv = jnp.sum(bias_parts, axis=(0, 1))
    chip_w_qkv = outer_sum(own_normed, d_proj_low, far_normed, far(d_proj_low))
    chip_both = jnp.concatenate([chip_w_out, chip_w_qkv], axis=1)
    chip_both, d_proj_next, act_next, grad_w_gate, grad_w_lin = lax.optimization_barrier((chip_both, d_proj_low, act_val, grad_w_gate, grad_w_lin))
    grad_both = scatter(chip_both)
    d_normed = lax.dot_general(d_proj_next, w_qkv, CONTRACT_COLS, preferred_element_type=jnp.float32)
    grad_attn_gain = jnp.sum(d_normed * hid_wide * inv_one, axis=0)
    scaled_one = d_normed * gain_one
    grad_hidden = (d_mid + inv_one * (scaled_one - hid_wide * inv_one * inv_one * jnp.mean(scaled_one * hid_wide, axis=-1, keepdims=True))).astype(jnp.bfloat16)
    output = (mid_wide + jnp.dot(act_next, w_down, preferred_element_type=jnp.float32)).astype(jnp.bfloat16)

    small = [lax.psum_scatter(value, axis, scatter_dimension=0, tiled=True) for value in (grad_attn_gain, grad_b_qkv, grad_mlp_gain)]
    whole = (batch_size, seq_len, width)
    grad_w_up = jnp.concatenate([grad_w_gate, grad_w_lin], axis=1)
    return output.reshape(whole), grad_hidden.reshape(whole), small[0], grad_both[:, width:], small[1], grad_both[:, :width], small[2], grad_w_up, grad_w_down


def solution(mesh):
    group_axis = mesh.axis_names[0]

    def local_step(*args):
        return layer_pass(group_axis, *args)

    row_spec = P(group_axis)
    return jax.shard_map(local_step, mesh=mesh, in_specs=(row_spec,) * 10, out_specs=(row_spec,) * 9, check_vma=False)
```

```python
import functools

import jax
import jax.numpy as jnp
from jax import lax
from jax.experimental import pallas as pl
from jax.experimental.pallas import tpu as pltpu
from jax.sharding import PartitionSpec as P


HEAD_DIM = 128
ROT_DIM = 64
ROPE_BASE = 10000.0
EPS = 1e-5
BLOCK = 128
PAD = 256
CONTRACT_ROWS = (((0,), (0,)), ((), ()))
CONTRACT_COLS = (((1,), (1,)), ((), ()))


def norm_scale(rows_in):
    return lax.rsqrt(jnp.mean(rows_in * rows_in, axis=-1, keepdims=True) + EPS)


def rope_tables(positions):
    inv_freq = 1.0 / (ROPE_BASE ** (jnp.arange(0, ROT_DIM, 2, dtype=jnp.float32) / ROT_DIM))
    lane_freq = jnp.concatenate([jnp.repeat(inv_freq, 2), jnp.zeros((HEAD_DIM - ROT_DIM,), jnp.float32)])
    angles = positions.reshape(-1, 1).astype(jnp.float32) * lane_freq
    signs = jnp.where(jnp.arange(HEAD_DIM) % 2 == 0, -1.0, 1.0)
    return jnp.cos(angles), jnp.sin(angles) * signs


def turn(head_vals, cos_t, sin_t):
    lane = lax.broadcasted_iota(jnp.int32, head_vals.shape, 1)
    partner = jnp.where(lane % 2 == 0, pltpu.roll(head_vals, HEAD_DIM - 1, 1), pltpu.roll(head_vals, 1, 1))
    return jnp.where(lane < ROT_DIM, head_vals * cos_t + partner * sin_t, head_vals)


def probs_t(keys, queries, first_row):
    scores = lax.dot_general(keys, queries, CONTRACT_COLS, preferred_element_type=jnp.float32) * HEAD_DIM ** -0.5
    key_at = lax.broadcasted_iota(jnp.int32, scores.shape, 0)
    query_at = lax.broadcasted_iota(jnp.int32, scores.shape, 1) % BLOCK + first_row
    scores = jnp.where(query_at >= key_at, scores, -1e30)
    weights = jnp.exp(scores - jnp.max(scores, axis=0, keepdims=True))
    return weights * (1.0 / jnp.sum(weights, axis=0, keepdims=True))


def attend_kernel(heads, kv_heads, z_ref, cos_ref, sin_ref, rot_ref, ctx_ref):
    seq = z_ref.shape[0]
    group = heads // kv_heads

    @pl.loop(0, heads + kv_heads)
    def _(j):
        at = pl.ds(pl.multiple_of(j * HEAD_DIM, HEAD_DIM), HEAD_DIM)
        rot_ref[:, at] = turn(z_ref[:, at], cos_ref[...], sin_ref[...]).astype(jnp.bfloat16)

    v_at = (heads + kv_heads) * HEAD_DIM
    rot_ref[:, v_at:] = z_ref[:, v_at:].astype(jnp.bfloat16)

    @pl.loop(0, kv_heads)
    def _(j):
        def head_at(n):
            return pl.ds(pl.multiple_of(n * HEAD_DIM, HEAD_DIM), HEAD_DIM)

        for first in range(0, seq, BLOCK):
            last = first + BLOCK
            queries = jnp.concatenate([rot_ref[first:last, head_at(j * group + g)] for g in range(group)], axis=0)
            probs = probs_t(rot_ref[:last, head_at(heads + j)], queries, first).astype(jnp.bfloat16)
            ctx = lax.dot_general(probs, rot_ref[:last, head_at(heads + kv_heads + j)], CONTRACT_ROWS, preferred_element_type=jnp.float32)
            for g in range(group):
                ctx_ref[first:last, head_at(j * group + g)] = ctx[g * BLOCK:(g + 1) * BLOCK].astype(jnp.bfloat16)


def attend_grad_kernel(heads, kv_heads, rot_ref, dctx_ref, cos_ref, sin_ref, dz_ref, bias_ref, dk_ref, dv_ref):
    seq = rot_ref.shape[0]
    group = heads // kv_heads

    @pl.loop(0, kv_heads)
    def _(j):
        def head_at(n):
            return pl.ds(pl.multiple_of(n * HEAD_DIM, HEAD_DIM), HEAD_DIM)

        def put(rows, head, value, fresh):
            dz_ref[rows, head_at(head)] = value.astype(jnp.bfloat16)
            part = jnp.sum(value.reshape(-1, 8, HEAD_DIM), axis=0)
            if fresh:
                bias_ref[0, :, head_at(head)] = part
            else:
                bias_ref[0, :, head_at(head)] += part

        dk_ref[...] = jnp.zeros_like(dk_ref)
        dv_ref[...] = jnp.zeros_like(dv_ref)
        for first in range(0, seq, BLOCK):
            last = first + BLOCK
            rows = slice(first, last)
            queries = jnp.concatenate([rot_ref[rows, head_at(j * group + g)] for g in range(group)], axis=0)
            dctx = jnp.concatenate([dctx_ref[rows, head_at(j * group + g)] for g in range(group)], axis=0)
            keys = rot_ref[:last, head_at(heads + j)]
            probs = probs_t(keys, queries, first)
            dv_ref[:last] += jnp.dot(probs.astype(jnp.bfloat16), dctx, preferred_element_type=jnp.float32)
            d_probs = lax.dot_general(rot_ref[:last, head_at(heads + kv_heads + j)], dctx, CONTRACT_COLS, preferred_element_type=jnp.float32)
            inner = jnp.sum(probs * d_probs, axis=0, keepdims=True)
            d_scores = (probs * (d_probs - inner) * HEAD_DIM ** -0.5).astype(jnp.bfloat16)
            dk_ref[:last] += jnp.dot(d_scores, queries, preferred_element_type=jnp.float32)
            d_query = lax.dot_general(d_scores, keys, CONTRACT_ROWS, preferred_element_type=jnp.float32)
            for g in range(group):
                turned = turn(d_query[g * BLOCK:(g + 1) * BLOCK], cos_ref[rows], -sin_ref[rows])
                put(rows, j * group + g, turned, first == 0)
        put(slice(0, seq), heads + j, turn(dk_ref[...], cos_ref[...], -sin_ref[...]), True)
        put(slice(0, seq), heads + kv_heads + j, dv_ref[...], True)


def rows_spec(seq, width):
    return pl.BlockSpec((seq, width), lambda i: (i, 0))


def attend(qkv_proj, cos_t, sin_t, seq, heads, kv_heads):
    tokens, width = qkv_proj.shape
    q_width = heads * HEAD_DIM
    return pl.pallas_call(
        functools.partial(attend_kernel, heads, kv_heads),
        grid=(tokens // seq,),
        in_specs=[rows_spec(seq, width), rows_spec(seq, HEAD_DIM), rows_spec(seq, HEAD_DIM)],
        out_specs=[rows_spec(seq, width), rows_spec(seq, q_width)],
        out_shape=[jax.ShapeDtypeStruct((tokens, width), jnp.bfloat16), jax.ShapeDtypeStruct((tokens, q_width), jnp.bfloat16)],
        cost_estimate=pl.CostEstimate(flops=30_000_000_000, bytes_accessed=40_000_000, transcendentals=10_000_000),
    )(qkv_proj, cos_t, sin_t)


def attend_grad(rot, d_context, cos_t, sin_t, seq, heads, kv_heads):
    tokens, width = rot.shape
    count = tokens // seq
    return pl.pallas_call(
        functools.partial(attend_grad_kernel, heads, kv_heads),
        grid=(count,),
        in_specs=[rows_spec(seq, width), rows_spec(seq, heads * HEAD_DIM), rows_spec(seq, HEAD_DIM), rows_spec(seq, HEAD_DIM)],
        out_specs=[rows_spec(seq, width), pl.BlockSpec((1, 8, width), lambda i: (i, 0, 0))],
        out_shape=[jax.ShapeDtypeStruct((tokens, width), jnp.bfloat16), jax.ShapeDtypeStruct((count, 8, width), jnp.float32)],
        scratch_shapes=[pltpu.VMEM((seq, HEAD_DIM), jnp.float32), pltpu.VMEM((seq, HEAD_DIM), jnp.float32)],
        cost_estimate=pl.CostEstimate(flops=60_000_000_000, bytes_accessed=40_000_000, transcendentals=10_000_000),
    )(rot, d_context, cos_t, sin_t)


def own_blocks(rows_in, width, bit):
    return jnp.concatenate([lax.dynamic_slice_in_dim(rows_in, (2 * i + bit) * width, width, axis=1) for i in range(8)], axis=1)


def outer_sum(own_left, own_right, far_left, far_right):
    first = lax.dot_general(own_left, own_right, CONTRACT_ROWS, preferred_element_type=jnp.float32)
    return first + lax.dot_general(far_left, far_right, CONTRACT_ROWS, preferred_element_type=jnp.float32)


def layer_pass(axis, hidden, positions, grad_y, attn_gain_s, w_qkv_s, b_qkv_s, w_out_s, mlp_gain_s, w_up_s, w_down_s):
    batch_size, seq_len, width = hidden.shape
    tokens = batch_size * seq_len
    count = lax.axis_size(axis)
    bit = lax.axis_index(axis) % 2
    swap = [(i, i ^ 1) for i in range(count)]
    groups = [list(range(0, count, 2)), list(range(1, count, 2))]

    def far(value):
        return lax.ppermute(value, axis, swap)

    def scatter(chip_sum):
        return lax.psum_scatter(chip_sum, axis, scatter_dimension=0, axis_index_groups=groups, tiled=True)

    def gather(shard):
        return lax.all_gather(shard, axis, axis=0, tiled=True)

    gain_rows = attn_gain_s.shape[0]
    bias_rows = b_qkv_s.shape[0]
    packed = jnp.concatenate([attn_gain_s, mlp_gain_s, b_qkv_s, jnp.zeros((4 * 128 - 2 * gain_rows - bias_rows,), jnp.bfloat16)])
    packed = lax.all_gather(packed.reshape(1, 4, 128), axis, axis=0, tiled=True).reshape(count, 512)
    attn_gain = packed[:, :gain_rows].reshape(width)
    mlp_gain = packed[:, gain_rows:2 * gain_rows].reshape(width)
    b_qkv = packed[:, 2 * gain_rows:2 * gain_rows + bias_rows].reshape(bias_rows * count)
    ff_width = w_down_s.shape[0] * count
    qkv_width = w_qkv_s.shape[1]
    w_attn = gather(jnp.concatenate([w_qkv_s, w_out_s, jnp.zeros((w_out_s.shape[0], PAD), jnp.bfloat16)], axis=1))
    w_qkv = w_attn[:, :qkv_width]
    w_out = w_attn[:, qkv_width:qkv_width + width]
    w_gate = gather(w_up_s[:, :ff_width])
    w_lin = gather(w_up_s[:, ff_width:])
    w_down = gather(w_down_s)

    q_width = w_out.shape[0]
    kv_width = (w_qkv.shape[1] - q_width) // 2
    heads = q_width // HEAD_DIM
    kv_heads = kv_width // HEAD_DIM
    h_rows = width // count
    ff_rows = ff_width // count
    cos_t, sin_t = rope_tables(positions)
    dy = grad_y.reshape(tokens, width)
    hid_wide = hidden.reshape(tokens, width).astype(jnp.float32)
    inv_one = norm_scale(hid_wide)
    gain_one = attn_gain.astype(jnp.float32)
    normed = (hid_wide * inv_one * gain_one).astype(jnp.bfloat16)
    far_dy = far(dy)
    own_normed = own_blocks(normed, h_rows, bit)
    far_normed = far(own_blocks(normed, h_rows, 1 - bit))
    qkv_proj = jnp.dot(normed, w_qkv, preferred_element_type=jnp.float32) + b_qkv.astype(jnp.float32)
    rot, context = attend(qkv_proj, cos_t, sin_t, seq_len, heads, kv_heads)
    mid_state = (hid_wide + jnp.dot(context, w_out, preferred_element_type=jnp.float32)).astype(jnp.bfloat16)
    mid_wide = mid_state.astype(jnp.float32)
    inv_two = norm_scale(mid_wide)
    gain_two = mlp_gain.astype(jnp.float32)
    mlp_in = (mid_wide * inv_two * gain_two).astype(jnp.bfloat16)
    own_mlp = own_blocks(mlp_in, h_rows, bit)
    far_mlp = far(own_blocks(mlp_in, h_rows, 1 - bit))
    own_ctx = own_blocks(context, q_width // count, bit)
    far_ctx = far(own_blocks(context, q_width // count, 1 - bit))
    up_gate = jnp.dot(mlp_in, w_gate, preferred_element_type=jnp.float32).astype(jnp.bfloat16)
    up_lin = jnp.dot(mlp_in, w_lin, preferred_element_type=jnp.float32).astype(jnp.bfloat16)
    gate_val = up_gate.astype(jnp.float32)
    lin_val = up_lin.astype(jnp.float32)
    sigmoid_gate = jax.nn.sigmoid(gate_val)
    act_val = (gate_val * sigmoid_gate * lin_val).astype(jnp.bfloat16)

    far_act = far(own_blocks(act_val, ff_rows, 1 - bit))
    own_act = own_blocks(act_val, ff_rows, bit)
    chip_w_down = outer_sum(own_act, dy, far_act, far_dy)
    chip_w_down, dy_next = lax.optimization_barrier((chip_w_down, dy))
    grad_w_down = scatter(chip_w_down)

    d_act = lax.dot_general(dy_next, w_down, CONTRACT_COLS, preferred_element_type=jnp.float32)
    d_gate = (d_act * lin_val * sigmoid_gate * (1.0 + gate_val * (1.0 - sigmoid_gate))).astype(jnp.bfloat16)
    d_lin = (d_act * gate_val * sigmoid_gate).astype(jnp.bfloat16)
    chip_w_gate = outer_sum(own_mlp, d_gate, far_mlp, far(d_gate))
    chip_w_lin = outer_sum(own_mlp, d_lin, far_mlp, far(d_lin))
    chip_w_gate, chip_w_lin, d_gate_next, d_lin_next, grad_w_down = lax.optimization_barrier((chip_w_gate, chip_w_lin, d_gate, d_lin, grad_w_down))
    grad_w_gate = scatter(chip_w_gate)
    grad_w_lin = scatter(chip_w_lin)

    d_mlp_in = lax.dot_general(d_gate_next, w_gate, CONTRACT_COLS, preferred_element_type=jnp.float32)
    d_mlp_in = d_mlp_in + lax.dot_general(d_lin_next, w_lin, CONTRACT_COLS, preferred_element_type=jnp.float32)
    grad_mlp_gain = jnp.sum(d_mlp_in * mid_wide * inv_two, axis=0)
    scaled_two = d_mlp_in * gain_two
    d_mid = dy.astype(jnp.float32) + inv_two * (scaled_two - mid_wide * inv_two * inv_two * jnp.mean(scaled_two * mid_wide, axis=-1, keepdims=True))
    d_mid_low = d_mid.astype(jnp.bfloat16)
    d_context = lax.dot_general(d_mid_low, w_out, CONTRACT_COLS, preferred_element_type=jnp.float32).astype(jnp.bfloat16)
    chip_w_out = outer_sum(own_ctx, d_mid_low, far_ctx, far(d_mid_low))
    d_proj_low, bias_parts = attend_grad(rot, d_context, cos_t, sin_t, seq_len, heads, kv_heads)
    grad_b_qkv = jnp.sum(bias_parts, axis=(0, 1))
    chip_w_qkv = outer_sum(own_normed, d_proj_low, far_normed, far(d_proj_low))
    chip_both = jnp.concatenate([chip_w_qkv, chip_w_out, jnp.zeros((chip_w_out.shape[0], PAD), jnp.float32)], axis=1)
    chip_both, d_proj_next, act_next, grad_w_gate, grad_w_lin = lax.optimization_barrier((chip_both, d_proj_low, act_val, grad_w_gate, grad_w_lin))
    grad_both = scatter(chip_both)
    d_normed = lax.dot_general(d_proj_next, w_qkv, CONTRACT_COLS, preferred_element_type=jnp.float32)
    grad_attn_gain = jnp.sum(d_normed * hid_wide * inv_one, axis=0)
    scaled_one = d_normed * gain_one
    grad_hidden = (d_mid + inv_one * (scaled_one - hid_wide * inv_one * inv_one * jnp.mean(scaled_one * hid_wide, axis=-1, keepdims=True))).astype(jnp.bfloat16)
    output = (mid_wide + jnp.dot(act_next, w_down, preferred_element_type=jnp.float32)).astype(jnp.bfloat16)

    small = [lax.psum_scatter(value, axis, scatter_dimension=0, tiled=True) for value in (grad_attn_gain, grad_b_qkv, grad_mlp_gain)]
    whole = (batch_size, seq_len, width)
    grad_w_up = jnp.concatenate([grad_w_gate, grad_w_lin], axis=1)
    return output.reshape(whole), grad_hidden.reshape(whole), small[0], grad_both[:, :qkv_width], small[1], grad_both[:, qkv_width:qkv_width + width], small[2], grad_w_up, grad_w_down


def solution(mesh):
    group_axis = mesh.axis_names[0]

    def local_step(*args):
        return layer_pass(group_axis, *args)

    row_spec = P(group_axis)
    return jax.shard_map(local_step, mesh=mesh, in_specs=(row_spec,) * 10, out_specs=(row_spec,) * 9, check_vma=False)
```

```python
import functools

import jax
import jax.numpy as jnp
from jax import lax
from jax.experimental import pallas as pl
from jax.experimental.pallas import tpu as pltpu
from jax.sharding import PartitionSpec as P


HEAD_DIM = 128
ROT_DIM = 64
ROPE_BASE = 10000.0
EPS = 1e-5
BLOCK = 128
PAD = 256
CONTRACT_ROWS = (((0,), (0,)), ((), ()))
CONTRACT_COLS = (((1,), (1,)), ((), ()))


def norm_scale(rows_in):
    return lax.rsqrt(jnp.mean(rows_in * rows_in, axis=-1, keepdims=True) + EPS)


def rope_tables(positions):
    inv_freq = 1.0 / (ROPE_BASE ** (jnp.arange(0, ROT_DIM, 2, dtype=jnp.float32) / ROT_DIM))
    lane_freq = jnp.concatenate([jnp.repeat(inv_freq, 2), jnp.zeros((HEAD_DIM - ROT_DIM,), jnp.float32)])
    angles = positions.reshape(-1, 1).astype(jnp.float32) * lane_freq
    signs = jnp.where(jnp.arange(HEAD_DIM) % 2 == 0, -1.0, 1.0)
    return jnp.cos(angles), jnp.sin(angles) * signs


def turn(head_vals, cos_t, sin_t):
    lane = lax.broadcasted_iota(jnp.int32, head_vals.shape, 1)
    partner = jnp.where(lane % 2 == 0, pltpu.roll(head_vals, HEAD_DIM - 1, 1), pltpu.roll(head_vals, 1, 1))
    return jnp.where(lane < ROT_DIM, head_vals * cos_t + partner * sin_t, head_vals)


def probs_t(keys, queries, first_row):
    scores = lax.dot_general(keys, queries, CONTRACT_COLS, preferred_element_type=jnp.float32) * HEAD_DIM ** -0.5
    key_at = lax.broadcasted_iota(jnp.int32, scores.shape, 0)
    query_at = lax.broadcasted_iota(jnp.int32, scores.shape, 1) % BLOCK + first_row
    scores = jnp.where(query_at >= key_at, scores, -1e30)
    weights = jnp.exp(scores - jnp.max(scores, axis=0, keepdims=True))
    return weights * (1.0 / jnp.sum(weights, axis=0, keepdims=True))


def attend_kernel(heads, kv_heads, z_ref, cos_ref, sin_ref, rot_ref, ctx_ref):
    seq = z_ref.shape[0]
    group = heads // kv_heads

    @pl.loop(0, heads + kv_heads)
    def _(j):
        at = pl.ds(pl.multiple_of(j * HEAD_DIM, HEAD_DIM), HEAD_DIM)
        rot_ref[:, at] = turn(z_ref[:, at], cos_ref[...], sin_ref[...]).astype(jnp.bfloat16)

    v_at = (heads + kv_heads) * HEAD_DIM
    rot_ref[:, v_at:] = z_ref[:, v_at:].astype(jnp.bfloat16)

    @pl.loop(0, kv_heads)
    def _(j):
        def head_at(n):
            return pl.ds(pl.multiple_of(n * HEAD_DIM, HEAD_DIM), HEAD_DIM)

        for first in range(0, seq, BLOCK):
            last = first + BLOCK
            queries = jnp.concatenate([rot_ref[first:last, head_at(j * group + g)] for g in range(group)], axis=0)
            probs = probs_t(rot_ref[:last, head_at(heads + j)], queries, first).astype(jnp.bfloat16)
            ctx = lax.dot_general(probs, rot_ref[:last, head_at(heads + kv_heads + j)], CONTRACT_ROWS, preferred_element_type=jnp.float32)
            for g in range(group):
                ctx_ref[first:last, head_at(j * group + g)] = ctx[g * BLOCK:(g + 1) * BLOCK].astype(jnp.bfloat16)


def attend_grad_kernel(heads, kv_heads, rot_ref, dctx_ref, cos_ref, sin_ref, dz_ref, bias_ref, dk_ref, dv_ref):
    seq = rot_ref.shape[0]
    group = heads // kv_heads

    @pl.loop(0, kv_heads)
    def _(j):
        def head_at(n):
            return pl.ds(pl.multiple_of(n * HEAD_DIM, HEAD_DIM), HEAD_DIM)

        def put(rows, head, value, fresh):
            dz_ref[rows, head_at(head)] = value.astype(jnp.bfloat16)
            part = jnp.sum(value.reshape(-1, 8, HEAD_DIM), axis=0)
            if fresh:
                bias_ref[0, :, head_at(head)] = part
            else:
                bias_ref[0, :, head_at(head)] += part

        dk_ref[...] = jnp.zeros_like(dk_ref)
        dv_ref[...] = jnp.zeros_like(dv_ref)
        for first in range(0, seq, BLOCK):
            last = first + BLOCK
            rows = slice(first, last)
            queries = jnp.concatenate([rot_ref[rows, head_at(j * group + g)] for g in range(group)], axis=0)
            dctx = jnp.concatenate([dctx_ref[rows, head_at(j * group + g)] for g in range(group)], axis=0)
            keys = rot_ref[:last, head_at(heads + j)]
            probs = probs_t(keys, queries, first)
            dv_ref[:last] += jnp.dot(probs.astype(jnp.bfloat16), dctx, preferred_element_type=jnp.float32)
            d_probs = lax.dot_general(rot_ref[:last, head_at(heads + kv_heads + j)], dctx, CONTRACT_COLS, preferred_element_type=jnp.float32)
            inner = jnp.sum(probs * d_probs, axis=0, keepdims=True)
            d_scores = (probs * (d_probs - inner) * HEAD_DIM ** -0.5).astype(jnp.bfloat16)
            dk_ref[:last] += jnp.dot(d_scores, queries, preferred_element_type=jnp.float32)
            d_query = lax.dot_general(d_scores, keys, CONTRACT_ROWS, preferred_element_type=jnp.float32)
            for g in range(group):
                turned = turn(d_query[g * BLOCK:(g + 1) * BLOCK], cos_ref[rows], -sin_ref[rows])
                put(rows, j * group + g, turned, first == 0)
        put(slice(0, seq), heads + j, turn(dk_ref[...], cos_ref[...], -sin_ref[...]), True)
        put(slice(0, seq), heads + kv_heads + j, dv_ref[...], True)


def rows_spec(seq, width):
    return pl.BlockSpec((seq, width), lambda i: (i, 0))


def attend(qkv_proj, cos_t, sin_t, seq, heads, kv_heads):
    tokens, width = qkv_proj.shape
    q_width = heads * HEAD_DIM
    return pl.pallas_call(
        functools.partial(attend_kernel, heads, kv_heads),
        grid=(tokens // seq,),
        in_specs=[rows_spec(seq, width), rows_spec(seq, HEAD_DIM), rows_spec(seq, HEAD_DIM)],
        out_specs=[rows_spec(seq, width), rows_spec(seq, q_width)],
        out_shape=[jax.ShapeDtypeStruct((tokens, width), jnp.bfloat16), jax.ShapeDtypeStruct((tokens, q_width), jnp.bfloat16)],
        cost_estimate=pl.CostEstimate(flops=30_000_000_000, bytes_accessed=40_000_000, transcendentals=10_000_000),
    )(qkv_proj, cos_t, sin_t)


def attend_grad(rot, d_context, cos_t, sin_t, seq, heads, kv_heads):
    tokens, width = rot.shape
    count = tokens // seq
    return pl.pallas_call(
        functools.partial(attend_grad_kernel, heads, kv_heads),
        grid=(count,),
        in_specs=[rows_spec(seq, width), rows_spec(seq, heads * HEAD_DIM), rows_spec(seq, HEAD_DIM), rows_spec(seq, HEAD_DIM)],
        out_specs=[rows_spec(seq, width), pl.BlockSpec((1, 8, width), lambda i: (i, 0, 0))],
        out_shape=[jax.ShapeDtypeStruct((tokens, width), jnp.bfloat16), jax.ShapeDtypeStruct((count, 8, width), jnp.float32)],
        scratch_shapes=[pltpu.VMEM((seq, HEAD_DIM), jnp.float32), pltpu.VMEM((seq, HEAD_DIM), jnp.float32)],
        cost_estimate=pl.CostEstimate(flops=60_000_000_000, bytes_accessed=40_000_000, transcendentals=10_000_000),
    )(rot, d_context, cos_t, sin_t)


def own_blocks(rows_in, width, bit):
    return jnp.concatenate([lax.dynamic_slice_in_dim(rows_in, (2 * i + bit) * width, width, axis=1) for i in range(8)], axis=1)


def split_kernel(pieces, bit_ref, rows_ref, own_ref, far_ref):
    piece = own_ref.shape[1] // pieces
    for bit in range(2):
        @pl.when(bit_ref[0] == bit)
        def _():
            for i in range(pieces):
                at = slice(i * piece, (i + 1) * piece)
                own_ref[:, at] = rows_ref[:, (2 * i + bit) * piece:(2 * i + bit + 1) * piece]
                far_ref[:, at] = rows_ref[:, (2 * i + 1 - bit) * piece:(2 * i + 2 - bit) * piece]


def split_blocks(rows_in, bit, step=256, pieces=8):
    tokens, width = rows_in.shape
    half = pl.BlockSpec((step, width // 2), lambda i, bit_ref: (i, 0))
    return pl.pallas_call(
        functools.partial(split_kernel, pieces),
        grid_spec=pltpu.PrefetchScalarGridSpec(
            num_scalar_prefetch=1,
            grid=(tokens // step,),
            in_specs=[pl.BlockSpec((step, width), lambda i, bit_ref: (i, 0))],
            out_specs=[half, half],
        ),
        out_shape=[jax.ShapeDtypeStruct((tokens, width // 2), rows_in.dtype)] * 2,
        cost_estimate=pl.CostEstimate(flops=10_000_000_000, bytes_accessed=4 * tokens * width, transcendentals=0),
    )(bit.reshape(1).astype(jnp.int32), rows_in)


def outer_sum(own_left, own_right, far_left, far_right):
    first = lax.dot_general(own_left, own_right, CONTRACT_ROWS, preferred_element_type=jnp.float32)
    return first + lax.dot_general(far_left, far_right, CONTRACT_ROWS, preferred_element_type=jnp.float32)


def layer_pass(axis, hidden, positions, grad_y, attn_gain_s, w_qkv_s, b_qkv_s, w_out_s, mlp_gain_s, w_up_s, w_down_s):
    batch_size, seq_len, width = hidden.shape
    tokens = batch_size * seq_len
    count = lax.axis_size(axis)
    bit = lax.axis_index(axis) % 2
    swap = [(i, i ^ 1) for i in range(count)]
    groups = [list(range(0, count, 2)), list(range(1, count, 2))]

    def far(value):
        return lax.ppermute(value, axis, swap)

    def scatter(chip_sum):
        return lax.psum_scatter(chip_sum, axis, scatter_dimension=0, axis_index_groups=groups, tiled=True)

    def gather(shard):
        return lax.all_gather(shard, axis, axis=0, tiled=True)

    gain_rows = attn_gain_s.shape[0]
    bias_rows = b_qkv_s.shape[0]
    packed = jnp.concatenate([attn_gain_s, mlp_gain_s, b_qkv_s, jnp.zeros((4 * 128 - 2 * gain_rows - bias_rows,), jnp.bfloat16)])
    packed = lax.all_gather(packed.reshape(1, 4, 128), axis, axis=0, tiled=True).reshape(count, 512)
    attn_gain = packed[:, :gain_rows].reshape(width)
    mlp_gain = packed[:, gain_rows:2 * gain_rows].reshape(width)
    b_qkv = packed[:, 2 * gain_rows:2 * gain_rows + bias_rows].reshape(bias_rows * count)
    ff_width = w_down_s.shape[0] * count
    qkv_width = w_qkv_s.shape[1]
    w_attn = gather(jnp.concatenate([w_qkv_s, w_out_s, jnp.zeros((w_out_s.shape[0], PAD), jnp.bfloat16)], axis=1))
    w_qkv = w_attn[:, :qkv_width]
    w_out = w_attn[:, qkv_width:qkv_width + width]
    w_gate = gather(w_up_s[:, :ff_width])
    w_lin = gather(w_up_s[:, ff_width:])
    w_down = gather(w_down_s)

    q_width = w_out.shape[0]
    kv_width = (w_qkv.shape[1] - q_width) // 2
    heads = q_width // HEAD_DIM
    kv_heads = kv_width // HEAD_DIM
    h_rows = width // count
    cos_t, sin_t = rope_tables(positions)
    dy = grad_y.reshape(tokens, width)
    hid_wide = hidden.reshape(tokens, width).astype(jnp.float32)
    inv_one = norm_scale(hid_wide)
    gain_one = attn_gain.astype(jnp.float32)
    normed = (hid_wide * inv_one * gain_one).astype(jnp.bfloat16)
    far_dy = far(dy)
    own_normed = own_blocks(normed, h_rows, bit)
    far_normed = far(own_blocks(normed, h_rows, 1 - bit))
    qkv_proj = jnp.dot(normed, w_qkv, preferred_element_type=jnp.float32) + b_qkv.astype(jnp.float32)
    rot, context = attend(qkv_proj, cos_t, sin_t, seq_len, heads, kv_heads)
    mid_state = (hid_wide + jnp.dot(context, w_out, preferred_element_type=jnp.float32)).astype(jnp.bfloat16)
    mid_wide = mid_state.astype(jnp.float32)
    inv_two = norm_scale(mid_wide)
    gain_two = mlp_gain.astype(jnp.float32)
    mlp_in = (mid_wide * inv_two * gain_two).astype(jnp.bfloat16)
    own_mlp = own_blocks(mlp_in, h_rows, bit)
    far_mlp = far(own_blocks(mlp_in, h_rows, 1 - bit))
    own_ctx = own_blocks(context, q_width // count, bit)
    far_ctx = far(own_blocks(context, q_width // count, 1 - bit))
    up_gate = jnp.dot(mlp_in, w_gate, preferred_element_type=jnp.float32).astype(jnp.bfloat16)
    up_lin = jnp.dot(mlp_in, w_lin, preferred_element_type=jnp.float32).astype(jnp.bfloat16)
    gate_val = up_gate.astype(jnp.float32)
    lin_val = up_lin.astype(jnp.float32)
    sigmoid_gate = jax.nn.sigmoid(gate_val)
    act_val = (gate_val * sigmoid_gate * lin_val).astype(jnp.bfloat16)

    own_act, far_act = split_blocks(act_val, bit)
    far_act = far(far_act)
    chip_w_down = outer_sum(own_act, dy, far_act, far_dy)
    chip_w_down, dy_next = lax.optimization_barrier((chip_w_down, dy))
    grad_w_down = scatter(chip_w_down)

    d_act = lax.dot_general(dy_next, w_down, CONTRACT_COLS, preferred_element_type=jnp.float32)
    d_gate = (d_act * lin_val * sigmoid_gate * (1.0 + gate_val * (1.0 - sigmoid_gate))).astype(jnp.bfloat16)
    d_lin = (d_act * gate_val * sigmoid_gate).astype(jnp.bfloat16)
    far_gate = far(d_gate)
    far_lin = far(d_lin)
    chip_w_gate = outer_sum(own_mlp, d_gate, far_mlp, far_gate)
    chip_w_gate, d_lin, far_lin, grad_w_down = lax.optimization_barrier((chip_w_gate, d_lin, far_lin, grad_w_down))
    chip_w_lin = outer_sum(own_mlp, d_lin, far_mlp, far_lin)
    chip_w_lin, d_gate_next, d_lin_next = lax.optimization_barrier((chip_w_lin, d_gate, d_lin))
    grad_w_gate = scatter(chip_w_gate)
    grad_w_lin = scatter(chip_w_lin)

    d_mlp_in = lax.dot_general(d_gate_next, w_gate, CONTRACT_COLS, preferred_element_type=jnp.float32)
    d_mlp_in = d_mlp_in + lax.dot_general(d_lin_next, w_lin, CONTRACT_COLS, preferred_element_type=jnp.float32)
    grad_mlp_gain = jnp.sum(d_mlp_in * mid_wide * inv_two, axis=0)
    scaled_two = d_mlp_in * gain_two
    d_mid = dy.astype(jnp.float32) + inv_two * (scaled_two - mid_wide * inv_two * inv_two * jnp.mean(scaled_two * mid_wide, axis=-1, keepdims=True))
    d_mid_low = d_mid.astype(jnp.bfloat16)
    d_context = lax.dot_general(d_mid_low, w_out, CONTRACT_COLS, preferred_element_type=jnp.float32).astype(jnp.bfloat16)
    chip_w_out = outer_sum(own_ctx, d_mid_low, far_ctx, far(d_mid_low))
    d_proj_low, bias_parts = attend_grad(rot, d_context, cos_t, sin_t, seq_len, heads, kv_heads)
    grad_b_qkv = jnp.sum(bias_parts, axis=(0, 1))
    chip_w_qkv = outer_sum(own_normed, d_proj_low, far_normed, far(d_proj_low))
    chip_both = jnp.concatenate([chip_w_qkv, chip_w_out, jnp.zeros((chip_w_out.shape[0], PAD), jnp.float32)], axis=1)
    chip_both, d_proj_next, act_next, grad_w_gate, grad_w_lin = lax.optimization_barrier((chip_both, d_proj_low, act_val, grad_w_gate, grad_w_lin))
    grad_both = scatter(chip_both)
    d_normed = lax.dot_general(d_proj_next, w_qkv, CONTRACT_COLS, preferred_element_type=jnp.float32)
    grad_attn_gain = jnp.sum(d_normed * hid_wide * inv_one, axis=0)
    scaled_one = d_normed * gain_one
    grad_hidden = (d_mid + inv_one * (scaled_one - hid_wide * inv_one * inv_one * jnp.mean(scaled_one * hid_wide, axis=-1, keepdims=True))).astype(jnp.bfloat16)
    output = (mid_wide + jnp.dot(act_next, w_down, preferred_element_type=jnp.float32)).astype(jnp.bfloat16)

    small = [lax.psum_scatter(value, axis, scatter_dimension=0, tiled=True) for value in (grad_attn_gain, grad_b_qkv, grad_mlp_gain)]
    whole = (batch_size, seq_len, width)
    grad_w_up = jnp.concatenate([grad_w_gate, grad_w_lin], axis=1)
    return output.reshape(whole), grad_hidden.reshape(whole), small[0], grad_both[:, :qkv_width], small[1], grad_both[:, qkv_width:qkv_width + width], small[2], grad_w_up, grad_w_down


def solution(mesh):
    group_axis = mesh.axis_names[0]

    def local_step(*args):
        return layer_pass(group_axis, *args)

    row_spec = P(group_axis)
    return jax.shard_map(local_step, mesh=mesh, in_specs=(row_spec,) * 10, out_specs=(row_spec,) * 9, check_vma=False)
```
